256 devices in a mesh: tm: 16 (over z, core), state: 16 (over y, x).
Axes of the slice: x: 4, y: 4, z: 8, core: 2. Of those that a mesh axis runs over, the one named last changes fastest.
Arguments:
- increments: bfloat16 [16, 2048, 128], P('tm', 'state'), may hold values from -4 to 4
- propagators: bfloat16 [16, 2048, 2048], P('tm', 'state'), may hold values from -1.1 to 1.1
- inv_var: float32 [16, 2048], P('tm', 'state'), may hold values from 0.25 to 2
Outputs:
- forward_state: bfloat16 [16, 2048, 128], P('tm', 'state')
- adjoint: bfloat16 [16, 2048, 128], P('tm', 'state')
The draws below stay inside these ranges and needn't reach their ends.
All inputs are finite; a program needn't handle non-finite values.
Results may differ from the reference program's by a relative error of at most 0.03.
Values may be sent and summed in bfloat16 or wider, within the bound.
No kernel may reach another device: no remote copies, remote signals or barrier semaphores. Data moves between devices by JAX's collectives and lax.ppermute only.
A program may use at most 64 MiB of HBM per device.

```python
import math
import jax
import jax.numpy as jnp
from jax import lax

SDIM = 2048
COLS = 128
WINDOWS = 16


def draw_propagators(key, part):
    first, second = jax.random.split(jax.random.fold_in(key, 11))
    diagonal = jax.random.uniform(first, (WINDOWS, SDIM), jnp.float32, 0.97, 1.0)
    remainder = jax.random.truncated_normal(second, -4.0, 4.0, (WINDOWS, SDIM, SDIM), jnp.float32) * (0.3 / math.sqrt(SDIM))
    identity = jnp.eye(SDIM, dtype=jnp.float32)
    return (remainder + diagonal[:, :, None] * identity[None]).astype(jnp.bfloat16)


def block_scale(own_key, extent, cuts, low, high):
    factor_of, own = 1.0, jax.random.fold_in(own_key, 6)
    for dim, parts in cuts:
        heights = jnp.exp(jax.random.uniform(jax.random.fold_in(own, dim), (parts,), jnp.float32, low / len(cuts), high / len(cuts)))
        factor_of = factor_of * jnp.repeat(heights, extent[dim] // parts).reshape([-1 if axis == dim else 1 for axis in range(len(extent))])
    return factor_of


def gaussian(stream_key, dims, width, most, cuts=(), kind=jnp.bfloat16):
    gain = block_scale(stream_key, dims, cuts, -0.22, 0.18) if cuts else 1.0
    drawn = jax.random.normal(stream_key, dims, jnp.float32) * width * gain
    return jnp.minimum(jnp.maximum(drawn, -most), most).astype(kind)


def setup_inputs(seed: int = 0) -> dict:
    streams_of = jax.random.split(jax.random.key(seed), 4)
    return {
        "increments": gaussian(streams_of[0], (WINDOWS, SDIM, COLS), 0.3, 4.0, ((0, 16), (1, 16))),
        "propagators": draw_propagators(jax.random.fold_in(streams_of[3], 71), 0),
        "inv_var": jnp.clip(jnp.exp(math.log(2.0) - 2.0794415 * jax.random.uniform(streams_of[2], (WINDOWS, SDIM), jnp.float32) ** block_scale(streams_of[2], (WINDOWS, SDIM), ((0, 16), (1, 16)), -0.2, 0.2)), 0.25, 2.0),
    }


def reference(increments, propagators, inv_var):
    def forward_step(previous, inputs):
        matrix, driving = inputs
        current = (jnp.dot(matrix, previous, preferred_element_type=jnp.float32) + driving.astype(jnp.float32)).astype(jnp.bfloat16)
        return current, current

    start = jnp.zeros(increments.shape[1:], jnp.bfloat16)
    finished, forward_state = lax.scan(forward_step, start, (propagators, increments))
    weighted = inv_var[:, :, None] * forward_state.astype(jnp.float32)

    def backward_step(carry, inputs):
        matrix, weight_now = inputs
        current = (weight_now + carry).astype(jnp.bfloat16)
        passed = lax.dot_general(matrix, current, (((0,), (0,)), ((), ())), preferred_element_type=jnp.float32)
        return passed, current

    blank = jnp.zeros(weighted.shape[1:], jnp.float32)
    leftover, adjoint = lax.scan(backward_step, blank, (propagators, weighted), reverse=True)
    return forward_state, adjoint
```

```python
import jax
import jax.numpy as jnp
from jax import lax
from jax.sharding import Mesh, PartitionSpec as P


Z, CORE, Y, X = 8, 2, 4, 4
PLANE = ("core", "y", "x")
ALL = ("z", "core", "y", "x")


def ring(block, axis, distance):
    n = lax.axis_size(axis)
    return lax.ppermute(block, axis, [(i, (i + distance) % n) for i in range(n)])


def z_hop(block, origin, target):
    size = CORE * Y * X
    return lax.ppermute(block, ALL, [(origin * size + i, target * size + i) for i in range(size)])


def other_core(block):
    return lax.ppermute(block, "core", [(0, 1), (1, 0)])


def put(buffer, piece, core, y, x):
    zero = jnp.int32(0)
    return lax.dynamic_update_slice(buffer, piece, (core, y, x, zero, zero))


def gathered(block, first, second):
    half = block.shape[0] // 2
    back, ahead = ring(block, first, 1), ring(block, first, -1)
    far = jnp.concatenate([ring(back[:half], first, 1), ring(ahead[half:], first, -1)], 0)
    return [(block, 0), (back, -1), (ahead, 1), (far, 2)]


def per_device(increments, propagators, inv_var):
    c, y, x = (lax.axis_index(a) for a in PLANE)
    z = lax.axis_index("z")
    matrix = propagators[0]
    rows = matrix.shape[0]
    wide = matrix.shape[1]
    half = wide // 2

    halves = []
    for part, (first, second) in enumerate((("x", "y"), ("y", "x"))):
        block = matrix[:, part * half:(part + 1) * half]
        at = {"x": x, "y": y}
        line = jnp.zeros((4, rows, half), jnp.bfloat16)
        for piece, off in gathered(block, first, second):
            line = lax.dynamic_update_slice(line, piece[None], ((at[first] + off) % 4, 0, 0))
        back, ahead = ring(line, second, 1), ring(line, second, -1)
        q0 = ring(back[:2], second, 1)
        q1 = ring(ahead[2:], second, -1)
        buffer = jnp.zeros((2, Y, X, rows, half), jnp.bfloat16)

        def place(buffer, piece, off, start, core):
            zero = jnp.int32(0)
            there = (at[second] + off) % 4
            if first == "x":
                return lax.dynamic_update_slice(buffer, piece[None, None], (core, there, start, zero, zero))
            return lax.dynamic_update_slice(buffer, piece[None, :, None], (core, start, there, zero, zero))

        for piece, off, start in ((line, 0, 0), (back, -1, 0), (ahead, 1, 0), (q0, 2, 0), (q1, 2, 2)):
            buffer = place(buffer, piece, off, jnp.int32(start), c)
            buffer = place(buffer, other_core(piece), off, jnp.int32(start), 1 - c)
        halves.append(buffer.reshape(2, wide, half))

    cols = increments.shape[2]
    own = cols // (CORE * Y * X)
    turned = increments[0].T.reshape(CORE * Y * X, own, rows)
    turned = lax.all_to_all(turned, PLANE, split_axis=0, concat_axis=0, tiled=True)
    driving = turned.reshape(2, Y * X, own, rows).transpose(0, 2, 1, 3).reshape(2, own, wide)
    driving = driving.astype(jnp.float32)
    weight = lax.all_gather(inv_var[0], PLANE, axis=0, tiled=True).reshape(2, 1, wide)

    def forward(window, state):
        total = driving[window]
        for part in range(2):
            total += lax.dot_general(state[:, part * half:(part + 1) * half], halves[part][window],
                                     (((1,), (1,)), ((), ())), preferred_element_type=jnp.float32)
        return total.astype(jnp.bfloat16)

    def backward(window, state):
        return jnp.concatenate([
            lax.dot_general(state, halves[part][window], (((1,), (0,)), ((), ())),
                            preferred_element_type=jnp.float32) for part in range(2)], 1)

    entering = jnp.zeros((own, wide), jnp.bfloat16)
    for step in range(Z):
        even = forward(0, entering)
        odd = forward(1, even)
        if step < Z - 1:
            arrived = z_hop(odd, step, step + 1)
            entering = jnp.where(z == step + 1, arrived, entering)

    weighted = [weight[0] * even.astype(jnp.float32), weight[1] * odd.astype(jnp.float32)]
    entering = jnp.zeros((own, wide), jnp.bfloat16)
    for step in reversed(range(Z)):
        adjoint_odd = (weighted[1] + entering.astype(jnp.float32)).astype(jnp.bfloat16)
        adjoint_even = (weighted[0] + backward(1, adjoint_odd)).astype(jnp.bfloat16)
        if step > 0:
            leaving = backward(0, adjoint_even).astype(jnp.bfloat16)
            arrived = z_hop(leaving, step, step - 1)
            entering = jnp.where(z == step - 1, arrived, entering)

    results = jnp.stack([jnp.stack([even, adjoint_even]), jnp.stack([odd, adjoint_odd])])
    results = results.reshape(2, 2, own, Y * X, rows).transpose(0, 3, 1, 2, 4).reshape(CORE * Y * X, 2, own, rows)
    results = lax.all_to_all(results, PLANE, split_axis=0, concat_axis=0, tiled=True)
    results = results.transpose(1, 3, 0, 2).reshape(2, rows, cols)
    return (results[:1], results[1:])


def solution(mesh):
    fine = Mesh(mesh.devices.reshape(Z, CORE, Y, X), ALL)
    tm, state = ("z", "core"), ("y", "x")
    in_specs = (P(tm, state, None), P(tm, state, None), P(tm, state))
    out_specs = (P(tm, state, None), P(tm, state, None))
    return jax.shard_map(per_device, mesh=fine, in_specs=in_specs, out_specs=out_specs, check_vma=False)
```

```python
import functools

import jax
import jax.numpy as jnp
from jax import lax
from jax.experimental import pallas as pl
from jax.experimental.pallas import tpu as pltpu
from jax.sharding import Mesh, PartitionSpec as P


Z, CORE, Y, X = 8, 2, 4, 4
PLANE = ("core", "y", "x")
ALL = ("z", "core", "y", "x")
MIB = 1 << 20


def ring(block, axis, distance):
    n = lax.axis_size(axis)
    return lax.ppermute(block, axis, [(i, (i + distance) % n) for i in range(n)])


def z_hop(block, origin, target):
    size = CORE * Y * X
    return lax.ppermute(block, ALL, [(origin * size + i, target * size + i) for i in range(size)])


def other_core(block):
    return lax.ppermute(block, "core", [(0, 1), (1, 0)])


def spread(block, axis, direction):
    behind, ahead = ring(block, axis, 1), ring(block, axis, -1)
    far = ring(behind, axis, 1) if direction > 0 else ring(ahead, axis, -1)
    return [block, behind, ahead, far]


OFFSETS = (0, -1, 1, 2)


def assemble_kernel(rows, width, fars, *refs):
    out, sems = refs[-2:]
    here = {axis: lax.axis_index(axis) for axis in PLANE}
    copies = []
    for owner in range(2):
        window = here["core"] if owner == 0 else 1 - here["core"]
        for quarter in range(4):
            first, second = ("x", "y") if quarter < 2 else ("y", "x")
            for j, far in enumerate(fars):
                piece = refs[(owner * 4 + quarter) * len(fars) + j]
                for i in range(4):
                    at = {first: (here[first] + OFFSETS[i] + 4) % 4, second: (here[second] + OFFSETS[far] + 4) % 4}
                    start = pl.multiple_of((at["y"] * X + at["x"]) * rows, rows)
                    copies.append(pltpu.make_async_copy(
                        piece.at[pl.ds(i * rows, rows), :],
                        out.at[window, pl.ds(start, rows), pl.ds(quarter * width, width)],
                        sems.at[len(copies)]))
    for copy in copies:
        copy.start()
    for copy in copies:
        copy.wait()


def assemble(pieces, wide, fars, whole=None):
    rows, width = pieces[0].shape[0] // 4, pieces[0].shape[1]
    in_specs = [pl.BlockSpec(memory_space=pltpu.HBM)] * len(pieces)
    kernel = functools.partial(assemble_kernel, rows, width, fars)
    operands, aliases = list(pieces), {}
    if whole is not None:
        in_specs.append(pl.BlockSpec(memory_space=pltpu.VMEM))
        operands.append(whole)
        aliases = {len(pieces): 0}
        inner = kernel
        kernel = lambda *refs: inner(*refs[:len(pieces)], *refs[len(pieces) + 1:])
    return pl.pallas_call(
        kernel,
        out_shape=jax.ShapeDtypeStruct((2, wide, wide), jnp.bfloat16),
        in_specs=in_specs,
        out_specs=pl.BlockSpec(memory_space=pltpu.VMEM),
        scratch_shapes=[pltpu.SemaphoreType.DMA((len(pieces) * 4,))],
        input_output_aliases=aliases,
        compiler_params=pltpu.CompilerParams(vmem_limit_bytes=2 * MIB),
        cost_estimate=pl.CostEstimate(flops=int(4e9), bytes_accessed=len(pieces) * MIB, transcendentals=0),
        name="assemble",
    )(*operands)


CHUNK = 512


def forward_kernel(entered, arrived, driving, whole, entering, even, odd):
    entering[...] = entered[...] + arrived[...]
    for window, (source, result) in enumerate(((entering, even), (even, odd))):
        state = source[...]

        @pl.loop(0, state.shape[1] // CHUNK)
        def _(n):
            part = pl.ds(pl.multiple_of(n * CHUNK, CHUNK), CHUNK)
            product = lax.dot_general(state, whole[window, part, :], (((1,), (1,)), ((), ())),
                                      preferred_element_type=jnp.float32)
            result[:, part] = (product + driving[window, :, part]).astype(result.dtype)


def backward_kernel(entered, arrived, weight, even, odd, whole, entering, adjoint_even, adjoint_odd, leaving):
    entering[...] = entered[...] + arrived[...]
    adjoint_odd[...] = (weight[1] * odd[...].astype(jnp.float32) + entering[...].astype(jnp.float32)).astype(odd.dtype)
    state = adjoint_odd[...]

    @pl.loop(0, state.shape[1] // CHUNK)
    def _(n):
        part = pl.ds(pl.multiple_of(n * CHUNK, CHUNK), CHUNK)
        carry = jnp.dot(state, whole[1, :, part], preferred_element_type=jnp.float32)
        own = weight[0, :, part] * even[:, part].astype(jnp.float32)
        adjoint_even[:, part] = (own + carry).astype(even.dtype)

    later = adjoint_even[...]

    @pl.loop(0, state.shape[1] // CHUNK)
    def _(n):
        part = pl.ds(pl.multiple_of(n * CHUNK, CHUNK), CHUNK)
        leaving[:, part] = jnp.dot(later, whole[0, :, part], preferred_element_type=jnp.float32).astype(leaving.dtype)


def chain_call(kernel, results, name, *operands):
    like = jax.ShapeDtypeStruct(operands[0].shape, operands[0].dtype)
    return pl.pallas_call(
        kernel,
        out_shape=[like] * results,
        in_specs=[pl.BlockSpec(memory_space=pltpu.VMEM)] * len(operands),
        out_specs=[pl.BlockSpec(memory_space=pltpu.VMEM)] * results,
        compiler_params=pltpu.CompilerParams(vmem_limit_bytes=2 * MIB),
        cost_estimate=pl.CostEstimate(flops=int(4e9), bytes_accessed=16 * MIB, transcendentals=0),
        name=name,
    )(*operands)


def per_device(increments, propagators, inv_var):
    matrix = propagators[0]
    rows, wide = matrix.shape
    width = wide // 4
    members = CORE * Y * X

    lines = []
    for quarter in range(4):
        axis = "x" if quarter < 2 else "y"
        block = matrix[:, quarter * width:(quarter + 1) * width]
        lines.append(jnp.concatenate(spread(block, axis, 1 - 2 * (quarter % 2)), 0))
    pieces = []
    for quarter in range(4):
        axis = "y" if quarter < 2 else "x"
        pieces += spread(lines[quarter], axis, 1 - 2 * (quarter % 2))

    cols = increments.shape[2]
    own = cols // members
    rest, parts = inv_var[0], []
    for _ in range(3):
        part = lax.reduce_precision(rest, 8, 7)
        parts.append(part.astype(jnp.bfloat16))
        rest = rest - part
    parts = jnp.broadcast_to(jnp.stack(parts)[None], (members, 3, rows))
    turned = jnp.concatenate([increments[0].T.reshape(members, own, rows), parts], 1)
    turned = lax.all_to_all(turned, PLANE, split_axis=0, concat_axis=0, tiled=True)
    turned = turned.reshape(2, Y * X, own + 3, rows).transpose(0, 2, 1, 3).reshape(2, own + 3, wide).astype(jnp.float32)
    driving = turned[:, :own]
    weight = turned[:, own:own + 1] + turned[:, own + 1:own + 2] + turned[:, own + 2:]

    pieces = pieces + [other_core(piece) for piece in pieces]
    near = [piece for i, piece in enumerate(pieces) if i % 4 < 3]
    whole = assemble(near, wide, (0, 1, 2))
    whole = assemble(pieces[3::4], wide, (3,), whole)

    nothing = jnp.zeros((own, wide), jnp.bfloat16)
    entering = arrived = nothing
    for step in range(Z):
        entering, even, odd = chain_call(forward_kernel, 3, "forward", entering, arrived, driving, whole)
        if step < Z - 1:
            arrived = z_hop(odd, step, step + 1)
    entering = arrived = nothing
    for step in reversed(range(Z)):
        entering, adjoint_even, adjoint_odd, leaving = chain_call(
            backward_kernel, 4, "backward", entering, arrived, weight, even, odd, whole)
        if step > 0:
            arrived = z_hop(leaving, step, step - 1)

    results = jnp.stack([jnp.stack([even, adjoint_even]), jnp.stack([odd, adjoint_odd])])
    results = results.reshape(2, 2, own, Y * X, rows).transpose(0, 3, 1, 2, 4).reshape(members, 2, own, rows)
    results = lax.all_to_all(results, PLANE, split_axis=0, concat_axis=0, tiled=True)
    results = results.transpose(1, 3, 0, 2).reshape(2, rows, cols)
    return (results[:1], results[1:])


def solution(mesh):
    fine = Mesh(mesh.devices.reshape(Z, CORE, Y, X), ALL)
    tm, state = ("z", "core"), ("y", "x")
    in_specs = (P(tm, state, None), P(tm, state, None), P(tm, state))
    out_specs = (P(tm, state, None), P(tm, state, None))
    return jax.shard_map(per_device, mesh=fine, in_specs=in_specs, out_specs=out_specs, check_vma=False)
```

```python
import functools

import jax
import jax.numpy as jnp
from jax import lax
from jax.experimental import pallas as pl
from jax.experimental.pallas import tpu as pltpu
from jax.sharding import Mesh, PartitionSpec as P


Z, CORE, Y, X = 8, 2, 4, 4
PLANE = ("core", "y", "x")
ALL = ("z", "core", "y", "x")
MIB = 1 << 20
F32, BF16 = jnp.float32, jnp.bfloat16
OFFSETS = (0, -1, 1, 2)
VMEM = pl.BlockSpec(memory_space=pltpu.VMEM)
HBM = pl.BlockSpec(memory_space=pltpu.HBM)


def ring(block, axis, distance):
    n = lax.axis_size(axis)
    return lax.ppermute(block, axis, [(i, (i + distance) % n) for i in range(n)])


def z_hop(block, origin, target):
    size = Y * X
    return lax.ppermute(block, ALL, [
        ((origin * CORE + core) * size + i, (target * CORE + 1 - core) * size + i) for core in range(CORE) for i in range(size)])


def own_half():
    return (lax.axis_index("core") + lax.axis_index("z")) % 2


def other_core(block):
    return lax.ppermute(block, "core", [(0, 1), (1, 0)])


def exchanged(messages, axis):
    dim = ("y", "x").index(axis)
    came = []
    for distance in range(4):
        message = lax.dynamic_index_in_dim(messages, (lax.axis_index(axis) + distance) % 4, dim, keepdims=False)
        came.append(ring(message, axis, distance) if distance else message)
    return jnp.stack(came, dim)


def call(kernel, results, operands, name, in_specs=None, flops=0, size=MIB, scratch=(), aliases=None):
    return pl.pallas_call(
        kernel,
        out_shape=results,
        in_specs=in_specs or [VMEM] * len(operands),
        out_specs=jax.tree.map(lambda _: VMEM, results),
        scratch_shapes=scratch,
        input_output_aliases=aliases or {},
        compiler_params=pltpu.CompilerParams(vmem_limit_bytes=4 * MIB),
        cost_estimate=pl.CostEstimate(flops=flops, bytes_accessed=size, transcendentals=0),
        name=name,
    )(*operands)


def shape(dims, dtype=BF16):
    return jax.ShapeDtypeStruct(dims, dtype)


def joined(left, right, low_half):
    lane = lax.broadcasted_iota(jnp.int32, left.shape, 1)
    if low_half:
        return jnp.where(lane < 64, left, pltpu.roll(right, 64, 1))
    return jnp.where(lane < 64, pltpu.roll(left, 64, 1), right)


def split_kernel(block, keep, give):
    rows, wide = block.shape
    half = wide // 2
    core, mine = lax.axis_index("core"), own_half()

    @pl.when(core == 1)
    def _():
        for target, which in ((keep, mine), (give, 1 - mine)):
            start = pl.ds(pl.multiple_of(which * 64, 64), 64)
            for side in range(2):
                target[side * 64:side * 64 + 64, :] = block[start, side * half:side * half + half]

    @pl.when(core == 0)
    def _():
        for u in range(wide // 256):
            left = block[:, 256 * u:256 * u + 128].astype(F32)
            right = block[:, 256 * u + 128:256 * u + 256].astype(F32)
            low, high = joined(left, right, True), joined(left, right, False)
            keep[:, 128 * u:128 * u + 128] = jnp.where(mine == 0, low, high).astype(BF16)
            give[:, 128 * u:128 * u + 128] = jnp.where(mine == 0, high, low).astype(BF16)


def assemble_kernel(fars, *refs):
    even, odd, even_turned, odd_turned, sems = refs[-5:]
    here = {axis: lax.axis_index(axis) for axis in PLANE}
    copies, taken = [], iter(refs)

    def copy(source, target):
        copies.append(pltpu.make_async_copy(source, target, sems.at[len(copies)]))

    def place(piece, row, column, part, columns, i, far):
        first, second = ("y", "x") if part == 0 else ("x", "y")
        at = {first: (here[first] + OFFSETS[i] + 4) % 4, second: (here[second] + OFFSETS[far] + 4) % 4}
        s = at["y"] * X + at["x"]
        if part == 0:
            copy(piece.at[pl.ds(row, 128), pl.ds(column, 512)],
                 even.at[pl.ds(pl.multiple_of(s * 128, 128), 128), pl.ds(columns, 512)])
        else:
            for side in range(2):
                copy(piece.at[pl.ds(row + side * 64, 64), pl.ds(column, 512)],
                     odd.at[pl.ds(pl.multiple_of(s * 64, 64), 64), pl.ds(side * 1024 + columns, 512)])

    for part in range(2):
        if len(fars) == 3:
            for far in fars:
                piece = next(taken)
                for columns in (0, 512):
                    place(piece, 0, columns, part, columns, 0, far)
        for columns in (0, 512):
            for far in fars:
                piece = next(taken)
                skipped = 1 if len(fars) == 3 else 0
                for i in range(skipped, 4):
                    place(piece, (i - skipped) * 128, 0, part, columns, i, far)
    for c in copies:
        c.start()
    for c in copies:
        c.wait()

    lowest, count = (-1, 3) if len(fars) == 3 else (2, 1)

    def turn(whole, turned, block):
        rows = pl.ds(pl.multiple_of(block * 128, 128), 128)
        for column in range(0, whole.shape[1], 512):
            turned[column:column + 512, rows] = whole[rows, column:column + 512].T

    @pl.loop(0, 4 * count)
    def _(n):
        turn(even, even_turned, n % 4 * X + (here["x"] + n // 4 + lowest + 4) % 4)

    @pl.loop(0, 2 * count)
    def _(n):
        turn(odd, odd_turned, (here["y"] + n // 2 + lowest + 4) % 4 * 2 + n % 2)


def assemble(pieces, fars, wide, before=()):
    def kernel(*refs):
        assemble_kernel(fars, *refs[:len(pieces)], *refs[len(pieces) + len(before):])

    tall, flat = shape((wide, wide // 2)), shape((wide // 2, wide))
    return call(
        kernel, [tall, flat, flat, tall], [*pieces, *before], "assemble",
        in_specs=[HBM] * len(pieces) + [VMEM] * len(before), flops=int(2e9), size=len(pieces) * MIB,
        scratch=[pltpu.SemaphoreType.DMA((96,))], aliases={len(pieces) + i: i for i in range(len(before))})


def prepare_kernel(messages, driving_even, driving_odd, weight_even, weight_odd, driving, weight):
    even_first, low = lax.axis_index("core") == 0, own_half() == 0
    y, x = lax.axis_index("y"), lax.axis_index("x")
    for i in range(Y):
        for j in range(X):
            s = (y - i + Y) % Y * X + (x - j + X) % X
            lanes = pl.ds(pl.multiple_of(s * 128, 128), 128)
            own, other = messages[i, j, 0].astype(F32), messages[i, j, 1].astype(F32)
            for block, to_driving, to_weight in ((jnp.where(even_first, own, other), driving_even, weight_even),
                                                 (jnp.where(even_first, other, own), driving, weight)):
                to_driving[:, lanes] = block[:8]
                to_weight[:, lanes] = jnp.broadcast_to(block[8:9] + block[9:10] + block[10:11], (8, 128))
    for source, target in ((driving, driving_odd), (weight, weight_odd)):
        for u in range(target.shape[1] // 128):
            left, right = source[:, 256 * u:256 * u + 128], source[:, 256 * u + 128:256 * u + 256]
            target[:, 128 * u:128 * u + 128] = jnp.where(low, joined(left, right, True), joined(left, right, False))


def forward_even_kernel(entered, arrived, even_turned, entering, partial):
    entering[...] = entered[...] + arrived[...]
    partial[...] = jnp.dot(entering[...], even_turned[...], preferred_element_type=F32)


def forward_odd_kernel(partial, other, driving_even, driving_odd, odd_turned, _, even, odd):
    even[...] = (partial[...] + other[...] + driving_even[...]).astype(BF16)
    odd[...] = (jnp.dot(even[...], odd_turned[...], preferred_element_type=F32) + driving_odd[...]).astype(BF16)


def backward_odd_kernel(entered, arrived, weight_odd, odd, odd_whole, _, entering, adjoint_odd, partial):
    entering[...] = entered[...] + arrived[...]
    adjoint_odd[...] = (weight_odd[...] * odd[...].astype(F32) + entering[...].astype(F32)).astype(BF16)
    partial[...] = jnp.dot(adjoint_odd[...], odd_whole[...], preferred_element_type=F32)


def backward_even_kernel(partial, other, weight_even, even, even_whole, _, adjoint_even, leaving):
    carry = partial[...] + other[...]
    adjoint_even[...] = (weight_even[...] * even[...].astype(F32) + carry).astype(BF16)
    leaving[...] = jnp.dot(adjoint_even[...], even_whole[...], preferred_element_type=F32).astype(BF16)


def pack_kernel(even, adjoint_even, odd, adjoint_odd, message):
    low = own_half() == 0
    blocks = even.shape[1] // 128

    def block(ref, i):
        return ref[:, 128 * i:128 * i + 128].astype(F32)

    for s in range(blocks):
        state, adjoint = block(even, s), block(adjoint_even, s)
        message[s] = jnp.where(low, joined(state, adjoint, True), joined(state, adjoint, False)).astype(BF16)
        message[blocks + s] = joined(block(odd, s // 2), block(adjoint_odd, s // 2), s % 2 == 0).astype(BF16)


def unpack_kernel(message, state, adjoint):
    for core in range(2):
        turned = message[core].astype(F32).T.astype(BF16)
        rows = pl.ds(pl.multiple_of((core + lax.axis_index("z")) % 2 * 64, 64), 64)
        state[0, rows, :] = turned[:64]
        adjoint[0, rows, :] = turned[64:]


def per_device(increments, propagators, inv_var):
    core = lax.axis_index("core")
    rows, wide = propagators.shape[1:]
    cols = increments.shape[2]
    members = Y * X
    own = cols // members
    half = wide // 2

    keep, give = call(split_kernel, [shape((rows, half))] * 2, [propagators[0]], "split")
    increments, inv_var, give = lax.optimization_barrier((increments, inv_var, give))
    taken = other_core(give)

    rest, parts = inv_var[0], []
    for _ in range(3):
        part = lax.reduce_precision(rest, 8, 7)
        parts.append(part.astype(BF16))
        rest = rest - part
    parts = jnp.broadcast_to(jnp.stack(parts)[None], (members, 3, rows))
    message = jnp.concatenate([increments[0].T.reshape(members, own, rows), parts], 1)
    messages = jnp.stack([message, other_core(message)], 1).reshape(Y, X, 2, own + 3, rows)
    messages, taken = lax.optimization_barrier((messages, taken))

    near, far = [], []
    for part, (first, second) in ((jnp.where(core == 0, keep, taken), ("y", "x")), (jnp.where(core == 0, taken, keep), ("x", "y"))):
        behind, ahead = ring(part, first, 1), ring(part, first, -1)
        if first == "y":
            messages, behind, ahead = lax.optimization_barrier((exchanged(messages, first), behind, ahead))
        own_behind, own_ahead = ring(part, second, 1), ring(part, second, -1)
        near += [part, own_behind, own_ahead]
        columns = [slice(0, half // 2), slice(half // 2, half)]
        beyond = [ring(behind[:, columns[0]], first, 1), ring(ahead[:, columns[1]], first, -1)]
        if first == "x":
            messages, *beyond = lax.optimization_barrier((exchanged(messages, first), *beyond))
        for side in range(2):
            line = jnp.concatenate([behind[:, columns[side]], ahead[:, columns[side]], beyond[side]], 0)
            after = [ring(line, second, 1), ring(line, second, -1)]
            near += [line, *after]
            source = (own_behind, own_ahead)[side][:, columns[side]]
            far.append(ring(jnp.concatenate([source, after[side]], 0), second, 1 - 2 * side))
    wide_f32, half_f32 = shape((own, wide), F32), shape((own, half), F32)
    driving_even, driving_odd, weight_even, weight_odd = call(
        prepare_kernel, [wide_f32, half_f32, wide_f32, half_f32], [messages], "prepare",
        scratch=[pltpu.VMEM((own, wide), F32)] * 2)

    before = assemble(near, (0, 1, 2), wide)
    even_whole, odd_whole, even_turned, odd_turned = assemble(far, (3,), wide, before)

    full, part = shape((own, wide)), shape((own, half))
    costs = {"flops": int(2e9), "size": 4 * MIB}
    nothing = jnp.zeros((own, half), BF16)
    entering = arrived = nothing
    even = jnp.zeros((own, wide), BF16)
    for step in range(Z):
        entering, partial = call(forward_even_kernel, [part, wide_f32], [entering, arrived, even_turned], "forward_even", **costs)
        even, odd = call(
            forward_odd_kernel, [full, part], [partial, other_core(partial), driving_even, driving_odd, odd_turned, even],
            "forward_odd", aliases={5: 0}, **costs)
        if step < Z - 1:
            arrived = z_hop(odd, step, step + 1)
    entering = arrived = nothing
    adjoint_even, adjoint_odd = jnp.zeros((own, wide), BF16), nothing
    for step in reversed(range(Z)):
        entering, adjoint_odd, partial = call(
            backward_odd_kernel, [part, part, wide_f32], [entering, arrived, weight_odd, odd, odd_whole, adjoint_odd],
            "backward_odd", aliases={5: 1}, **costs)
        adjoint_even, leaving = call(
            backward_even_kernel, [full, part], [partial, other_core(partial), weight_even, even, even_whole, adjoint_even],
            "backward_even", aliases={5: 0}, **costs)
        if step > 0:
            arrived = z_hop(leaving, step, step - 1)

    message = call(pack_kernel, shape((CORE * members, own, rows)), [even, adjoint_even, odd, adjoint_odd], "pack")
    message = lax.all_to_all(message, PLANE, split_axis=0, concat_axis=0, tiled=True)
    block = shape((1, rows, cols))
    return tuple(call(unpack_kernel, [block, block], [message.reshape(CORE, cols, rows)], "unpack"))


def solution(mesh):
    fine = Mesh(mesh.devices.reshape(Z, CORE, Y, X), ALL)
    tm, state = ("z", "core"), ("y", "x")
    in_specs = (P(tm, state, None), P(tm, state, None), P(tm, state))
    out_specs = (P(tm, state, None), P(tm, state, None))
    return jax.shard_map(per_device, mesh=fine, in_specs=in_specs, out_specs=out_specs, check_vma=False)
```

```python
import functools

import jax
import jax.numpy as jnp
from jax import lax
from jax.experimental import pallas as pl
from jax.experimental.pallas import tpu as pltpu
from jax.sharding import Mesh, PartitionSpec as P


Z, CORE, Y, X = 8, 2, 4, 4
PLANE = ("core", "y", "x")
ALL = ("z", "core", "y", "x")
MIB = 1 << 20
F32, BF16 = jnp.float32, jnp.bfloat16
OFFSETS = (0, -1, 1, 2)
VMEM = pl.BlockSpec(memory_space=pltpu.VMEM)
HBM = pl.BlockSpec(memory_space=pltpu.HBM)


def ring(block, axis, distance):
    n = lax.axis_size(axis)
    return lax.ppermute(block, axis, [(i, (i + distance) % n) for i in range(n)])


def z_hop(block, origin, target):
    size = Y * X
    return lax.ppermute(block, ALL, [
        ((origin * CORE + core) * size + i, (target * CORE + 1 - core) * size + i) for core in range(CORE) for i in range(size)])


def own_half():
    return (lax.axis_index("core") + lax.axis_index("z")) % 2


def other_core(block):
    return lax.ppermute(block, "core", [(0, 1), (1, 0)])


def exchanged(messages, axis):
    dim = ("y", "x").index(axis)
    came = []
    for distance in range(4):
        message = lax.dynamic_index_in_dim(messages, (lax.axis_index(axis) + distance) % 4, dim, keepdims=False)
        came.append(ring(message, axis, distance) if distance else message)
    return came


def call(kernel, results, operands, name, in_specs=None, flops=0, size=MIB, scratch=(), aliases=None):
    return pl.pallas_call(
        kernel,
        out_shape=results,
        in_specs=in_specs or [VMEM] * len(operands),
        out_specs=jax.tree.map(lambda _: VMEM, results),
        scratch_shapes=scratch,
        input_output_aliases=aliases or {},
        compiler_params=pltpu.CompilerParams(vmem_limit_bytes=4 * MIB),
        cost_estimate=pl.CostEstimate(flops=flops, bytes_accessed=size, transcendentals=0),
        name=name,
    )(*operands)


def shape(dims, dtype=BF16):
    return jax.ShapeDtypeStruct(dims, dtype)


def joined(left, right, low_half):
    lane = lax.broadcasted_iota(jnp.int32, left.shape, 1)
    if low_half:
        return jnp.where(lane < 64, left, pltpu.roll(right, 64, 1))
    return jnp.where(lane < 64, pltpu.roll(left, 64, 1), right)


def split_kernel(block, keep, give):
    rows, wide = block.shape
    half = wide // 2
    core, mine = lax.axis_index("core"), own_half()

    @pl.when(core == 1)
    def _():
        for target, which in ((keep, mine), (give, 1 - mine)):
            start = pl.ds(pl.multiple_of(which * 64, 64), 64)
            for side in range(2):
                target[side * 64:side * 64 + 64, :] = block[start, side * half:side * half + half]

    @pl.when(core == 0)
    def _():
        for u in range(wide // 256):
            left = block[:, 256 * u:256 * u + 128].astype(F32)
            right = block[:, 256 * u + 128:256 * u + 256].astype(F32)
            low, high = joined(left, right, True), joined(left, right, False)
            keep[:, 128 * u:128 * u + 128] = jnp.where(mine == 0, low, high).astype(BF16)
            give[:, 128 * u:128 * u + 128] = jnp.where(mine == 0, high, low).astype(BF16)


def assemble_kernel(fars, *refs):
    even, odd, even_turned, odd_turned, sems = refs[-5:]
    here = {axis: lax.axis_index(axis) for axis in PLANE}
    copies = []

    def copy(source, target):
        copies.append(pltpu.make_async_copy(source, target, sems.at[len(copies)]))

    for quarter in range(4):
        first, second = ("x", "y") if quarter < 2 else ("y", "x")
        columns = (quarter % 2) * 512
        for j, far in enumerate(fars):
            piece = refs[quarter * len(fars) + j]
            for i in range(4):
                at = {first: (here[first] + OFFSETS[i] + 4) % 4, second: (here[second] + OFFSETS[far] + 4) % 4}
                s = at["y"] * X + at["x"]
                if quarter < 2:
                    for side in range(2):
                        copy(piece.at[pl.ds(i * 128 + side * 64, 64), :],
                             odd.at[pl.ds(pl.multiple_of(s * 64, 64), 64), pl.ds(side * 1024 + columns, 512)])
                else:
                    copy(piece.at[pl.ds(i * 128, 128), :],
                         even.at[pl.ds(pl.multiple_of(s * 128, 128), 128), pl.ds(columns, 512)])
    for c in copies:
        c.start()
    for c in copies:
        c.wait()

    lowest, count = (-1, 3) if len(fars) == 3 else (2, 1)

    def turn(whole, turned, block):
        rows = pl.ds(pl.multiple_of(block * 128, 128), 128)
        for column in range(0, whole.shape[1], 512):
            turned[column:column + 512, rows] = whole[rows, column:column + 512].T

    @pl.loop(0, 4 * count)
    def _(n):
        turn(even, even_turned, n % 4 * X + (here["x"] + n // 4 + lowest + 4) % 4)

    @pl.loop(0, 2 * count)
    def _(n):
        turn(odd, odd_turned, (here["y"] + n // 2 + lowest + 4) % 4 * 2 + n % 2)


def assemble(pieces, fars, wide, before=()):
    def kernel(*refs):
        assemble_kernel(fars, *refs[:len(pieces)], *refs[len(pieces) + len(before):])

    tall, flat = shape((wide, wide // 2)), shape((wide // 2, wide))
    return call(
        kernel, [tall, flat, flat, tall], [*pieces, *before], "assemble",
        in_specs=[HBM] * len(pieces) + [VMEM] * len(before), flops=int(2e9), size=len(pieces) * MIB,
        scratch=[pltpu.SemaphoreType.DMA((len(pieces) * 6,))], aliases={len(pieces) + i: i for i in range(len(before))})


def prepare_kernel(messages, driving_even, driving_odd, weight_even, weight_odd, driving, weight):
    even_first, low = lax.axis_index("core") == 0, own_half() == 0
    y, x = lax.axis_index("y"), lax.axis_index("x")
    for i in range(Y):
        for j in range(X):
            s = (y - i + Y) % Y * X + (x - j + X) % X
            lanes = pl.ds(pl.multiple_of(s * 128, 128), 128)
            own, other = messages[i, j, 0].astype(F32), messages[i, j, 1].astype(F32)
            for block, to_driving, to_weight in ((jnp.where(even_first, own, other), driving_even, weight_even),
                                                 (jnp.where(even_first, other, own), driving, weight)):
                to_driving[:, lanes] = block[:8]
                to_weight[:, lanes] = jnp.broadcast_to(block[8:9] + block[9:10] + block[10:11], (8, 128))
    for source, target in ((driving, driving_odd), (weight, weight_odd)):
        for u in range(target.shape[1] // 128):
            left, right = source[:, 256 * u:256 * u + 128], source[:, 256 * u + 128:256 * u + 256]
            target[:, 128 * u:128 * u + 128] = jnp.where(low, joined(left, right, True), joined(left, right, False))


def forward_even_kernel(entered, arrived, even_turned, entering, partial):
    entering[...] = entered[...] + arrived[...]
    partial[...] = jnp.dot(entering[...], even_turned[...], preferred_element_type=F32)


def forward_odd_kernel(partial, other, driving_even, driving_odd, odd_turned, _, even, odd):
    even[...] = (partial[...] + other[...] + driving_even[...]).astype(BF16)
    odd[...] = (jnp.dot(even[...], odd_turned[...], preferred_element_type=F32) + driving_odd[...]).astype(BF16)


def backward_odd_kernel(entered, arrived, weight_odd, odd, odd_whole, _, entering, adjoint_odd, partial):
    entering[...] = entered[...] + arrived[...]
    adjoint_odd[...] = (weight_odd[...] * odd[...].astype(F32) + entering[...].astype(F32)).astype(BF16)
    partial[...] = jnp.dot(adjoint_odd[...], odd_whole[...], preferred_element_type=F32)


def backward_even_kernel(partial, other, weight_even, even, even_whole, _, adjoint_even, leaving):
    carry = partial[...] + other[...]
    adjoint_even[...] = (weight_even[...] * even[...].astype(F32) + carry).astype(BF16)
    leaving[...] = jnp.dot(adjoint_even[...], even_whole[...], preferred_element_type=F32).astype(BF16)


def pack_kernel(even, adjoint_even, odd, adjoint_odd, message):
    low = own_half() == 0
    blocks = even.shape[1] // 128

    def block(ref, i):
        return ref[:, 128 * i:128 * i + 128].astype(F32)

    for s in range(blocks):
        state, adjoint = block(even, s), block(adjoint_even, s)
        message[s] = jnp.where(low, joined(state, adjoint, True), joined(state, adjoint, False)).astype(BF16)
        message[blocks + s] = joined(block(odd, s // 2), block(adjoint_odd, s // 2), s % 2 == 0).astype(BF16)


def unpack_kernel(message, state, adjoint):
    for core in range(2):
        turned = message[core].astype(F32).T.astype(BF16)
        rows = pl.ds(pl.multiple_of((core + lax.axis_index("z")) % 2 * 64, 64), 64)
        state[0, rows, :] = turned[:64]
        adjoint[0, rows, :] = turned[64:]


def per_device(increments, propagators, inv_var):
    core = lax.axis_index("core")
    rows, wide = propagators.shape[1:]
    cols = increments.shape[2]
    members = Y * X
    own = cols // members
    half = wide // 2

    keep, give = call(split_kernel, [shape((rows, half))] * 2, [propagators[0]], "split")
    increments, inv_var, give = lax.optimization_barrier((increments, inv_var, give))
    taken = other_core(give)

    rest, parts = inv_var[0], []
    for _ in range(3):
        part = lax.reduce_precision(rest, 8, 7)
        parts.append(part.astype(BF16))
        rest = rest - part
    parts = jnp.broadcast_to(jnp.stack(parts)[None], (members, 3, rows))
    message = jnp.concatenate([increments[0].T.reshape(members, own, rows), parts], 1)
    messages = jnp.stack([message, other_core(message)], 1).reshape(Y, X, 2, own + 3, rows)
    messages, taken = lax.optimization_barrier((messages, taken))
    near, far = [], []
    for part, (first, second) in ((jnp.where(core == 0, keep, taken), ("y", "x")), (jnp.where(core == 0, taken, keep), ("x", "y"))):
        behind, ahead = ring(part, first, 1), ring(part, first, -1)
        columns = [slice(0, half // 2), slice(half // 2, half)]
        beyond = [ring(behind[:, columns[0]], first, 1), ring(ahead[:, columns[1]], first, -1)]
        for side in range(2):
            line = jnp.concatenate([block[:, columns[side]] for block in (part, behind, ahead)] + [beyond[side]], 0)
            if first == "x" and side == 1:
                messages, line = lax.optimization_barrier((messages, line))
                came = exchanged(messages, "y")
            after = [ring(line, second, 1), ring(line, second, -1)]
            near.append([line, *after])
            far.append(ring(after[side], second, 1 - 2 * side))
    near, far = near[2:] + near[:2], far[2:] + far[:2]
    before = assemble([piece for group in near for piece in group], (0, 1, 2), wide)
    came, before = lax.optimization_barrier((came, before))
    messages = jnp.stack(exchanged(jnp.stack(came, 0), "x"), 1)
    wide_f32, half_f32 = shape((own, wide), F32), shape((own, half), F32)
    driving_even, driving_odd, weight_even, weight_odd = call(
        prepare_kernel, [wide_f32, half_f32, wide_f32, half_f32], [messages], "prepare",
        scratch=[pltpu.VMEM((own, wide), F32)] * 2)
    even_whole, odd_whole, even_turned, odd_turned = assemble(far, (3,), wide, before)

    full, part = shape((own, wide)), shape((own, half))
    costs = {"flops": int(2e9), "size": 4 * MIB}
    nothing = jnp.zeros((own, half), BF16)
    entering = arrived = nothing
    even = jnp.zeros((own, wide), BF16)
    for step in range(Z):
        entering, partial = call(forward_even_kernel, [part, wide_f32], [entering, arrived, even_turned], "forward_even", **costs)
        even, odd = call(
            forward_odd_kernel, [full, part], [partial, other_core(partial), driving_even, driving_odd, odd_turned, even],
            "forward_odd", aliases={5: 0}, **costs)
        if step < Z - 1:
            arrived = z_hop(odd, step, step + 1)
    entering = arrived = nothing
    adjoint_even, adjoint_odd = jnp.zeros((own, wide), BF16), nothing
    for step in reversed(range(Z)):
        entering, adjoint_odd, partial = call(
            backward_odd_kernel, [part, part, wide_f32], [entering, arrived, weight_odd, odd, odd_whole, adjoint_odd],
            "backward_odd", aliases={5: 1}, **costs)
        adjoint_even, leaving = call(
            backward_even_kernel, [full, part], [partial, other_core(partial), weight_even, even, even_whole, adjoint_even],
            "backward_even", aliases={5: 0}, **costs)
        if step > 0:
            arrived = z_hop(leaving, step, step - 1)

    message = call(pack_kernel, shape((CORE * members, own, rows)), [even, adjoint_even, odd, adjoint_odd], "pack")
    message = lax.all_to_all(message, PLANE, split_axis=0, concat_axis=0, tiled=True)
    block = shape((1, rows, cols))
    return tuple(call(unpack_kernel, [block, block], [message.reshape(CORE, cols, rows)], "unpack"))


def solution(mesh):
    fine = Mesh(mesh.devices.reshape(Z, CORE, Y, X), ALL)
    tm, state = ("z", "core"), ("y", "x")
    in_specs = (P(tm, state, None), P(tm, state, None), P(tm, state))
    out_specs = (P(tm, state, None), P(tm, state, None))
    return jax.shard_map(per_device, mesh=fine, in_specs=in_specs, out_specs=out_specs, check_vma=False)
```

```python
import functools

import jax
import jax.numpy as jnp
from jax import lax
from jax.experimental import pallas as pl
from jax.experimental.pallas import tpu as pltpu
from jax.sharding import Mesh, PartitionSpec as P


Z, CORE, Y, X = 8, 2, 4, 4
PLANE = ("core", "y", "x")
ALL = ("z", "core", "y", "x")
MIB = 1 << 20
F32, BF16 = jnp.float32, jnp.bfloat16
OFFSETS = (0, -1, 1, 2)
VMEM = pl.BlockSpec(memory_space=pltpu.VMEM)
HBM = pl.BlockSpec(memory_space=pltpu.HBM)


def ring(block, axis, distance):
    n = lax.axis_size(axis)
    return lax.ppermute(block, axis, [(i, (i + distance) % n) for i in range(n)])


def z_hop(block, origin, target):
    size = Y * X
    return lax.ppermute(block, ALL, [
        ((origin * CORE + core) * size + i, (target * CORE + 1 - core) * size + i) for core in range(CORE) for i in range(size)])


def own_half():
    return (lax.axis_index("core") + lax.axis_index("z")) % 2


def other_core(block):
    return lax.ppermute(block, "core", [(0, 1), (1, 0)])


def exchanged(messages, axis):
    dim = ("y", "x").index(axis)
    came = []
    for distance in range(4):
        message = lax.dynamic_index_in_dim(messages, (lax.axis_index(axis) + distance) % 4, dim, keepdims=False)
        came.append(ring(message, axis, distance) if distance else message)
    return came


def call(kernel, results, operands, name, in_specs=None, flops=0, size=MIB, scratch=(), aliases=None):
    return pl.pallas_call(
        kernel,
        out_shape=results,
        in_specs=in_specs or [VMEM] * len(operands),
        out_specs=jax.tree.map(lambda _: VMEM, results),
        scratch_shapes=scratch,
        input_output_aliases=aliases or {},
        compiler_params=pltpu.CompilerParams(vmem_limit_bytes=4 * MIB),
        cost_estimate=pl.CostEstimate(flops=flops, bytes_accessed=size, transcendentals=0),
        name=name,
    )(*operands)


def shape(dims, dtype=BF16):
    return jax.ShapeDtypeStruct(dims, dtype)


def joined(left, right, low_half):
    lane = lax.broadcasted_iota(jnp.int32, left.shape, 1)
    if low_half:
        return jnp.where(lane < 64, left, pltpu.roll(right, 64, 1))
    return jnp.where(lane < 64, pltpu.roll(left, 64, 1), right)


def split_kernel(block, keep, give):
    rows, wide = block.shape
    half = wide // 2
    core, mine = lax.axis_index("core"), own_half()

    @pl.when(core == 1)
    def _():
        for target, which in ((keep, mine), (give, 1 - mine)):
            start = pl.ds(pl.multiple_of(which * 64, 64), 64)
            for side in range(2):
                target[side * 64:side * 64 + 64, :] = block[start, side * half:side * half + half]

    @pl.when(core == 0)
    def _():
        for u in range(wide // 256):
            left = block[:, 256 * u:256 * u + 128].astype(F32)
            right = block[:, 256 * u + 128:256 * u + 256].astype(F32)
            low, high = joined(left, right, True), joined(left, right, False)
            keep[:, 128 * u:128 * u + 128] = jnp.where(mine == 0, low, high).astype(BF16)
            give[:, 128 * u:128 * u + 128] = jnp.where(mine == 0, high, low).astype(BF16)


def assemble_kernel(fars, *refs):
    even, odd, even_turned, odd_turned, sems = refs[-5:]
    here = {axis: lax.axis_index(axis) for axis in PLANE}
    copies = []

    def copy(source, target):
        copies.append(pltpu.make_async_copy(source, target, sems.at[len(copies)]))

    for quarter in range(4):
        first, second = ("x", "y") if quarter < 2 else ("y", "x")
        columns = (quarter % 2) * 512
        for j, far in enumerate(fars):
            piece = refs[quarter * len(fars) + j]
            for i in range(4):
                at = {first: (here[first] + OFFSETS[i] + 4) % 4, second: (here[second] + OFFSETS[far] + 4) % 4}
                s = at["y"] * X + at["x"]
                if quarter < 2:
                    for side in range(2):
                        copy(piece.at[pl.ds(i * 128 + side * 64, 64), :],
                             odd.at[pl.ds(pl.multiple_of(s * 64, 64), 64), pl.ds(side * 1024 + columns, 512)])
                else:
                    copy(piece.at[pl.ds(i * 128, 128), :],
                         even.at[pl.ds(pl.multiple_of(s * 128, 128), 128), pl.ds(columns, 512)])
    for c in copies:
        c.start()
    for c in copies:
        c.wait()

    lowest, count = (-1, 3) if len(fars) == 3 else (2, 1)

    def turn(whole, turned, block):
        rows = pl.ds(pl.multiple_of(block * 128, 128), 128)
        for column in range(0, whole.shape[1], 512):
            turned[column:column + 512, rows] = whole[rows, column:column + 512].T

    @pl.loop(0, 4 * count)
    def _(n):
        turn(even, even_turned, n % 4 * X + (here["x"] + n // 4 + lowest + 4) % 4)

    @pl.loop(0, 2 * count)
    def _(n):
        turn(odd, odd_turned, (here["y"] + n // 2 + lowest + 4) % 4 * 2 + n % 2)


def assemble(pieces, fars, wide, before=()):
    def kernel(*refs):
        assemble_kernel(fars, *refs[:len(pieces)], *refs[len(pieces) + len(before):])

    tall, flat = shape((wide, wide // 2)), shape((wide // 2, wide))
    return call(
        kernel, [tall, flat, flat, tall], [*pieces, *before], "assemble",
        in_specs=[HBM] * len(pieces) + [VMEM] * len(before), flops=int(2e9), size=len(pieces) * MIB,
        scratch=[pltpu.SemaphoreType.DMA((len(pieces) * 6,))], aliases={len(pieces) + i: i for i in range(len(before))})


def prepare_kernel(messages, driving_even, driving_odd, weight_even, weight_odd, driving, weight):
    even_first, low = lax.axis_index("core") == 0, own_half() == 0
    y, x = lax.axis_index("y"), lax.axis_index("x")
    for i in range(Y):
        for j in range(X):
            s = (y - i + Y) % Y * X + (x - j + X) % X
            lanes = pl.ds(pl.multiple_of(s * 128, 128), 128)
            own, other = messages[i, j, 0].astype(F32), messages[i, j, 1].astype(F32)
            for block, to_driving, to_weight in ((jnp.where(even_first, own, other), driving_even, weight_even),
                                                 (jnp.where(even_first, other, own), driving, weight)):
                to_driving[:, lanes] = block[:8]
                to_weight[:, lanes] = jnp.broadcast_to(block[8:9] + block[9:10] + block[10:11], (8, 128))
    for source, target in ((driving, driving_odd), (weight, weight_odd)):
        for u in range(target.shape[1] // 128):
            left, right = source[:, 256 * u:256 * u + 128], source[:, 256 * u + 128:256 * u + 256]
            target[:, 128 * u:128 * u + 128] = jnp.where(low, joined(left, right, True), joined(left, right, False))


def forward_even_kernel(entered, arrived, even_turned, entering, partial):
    entering[...] = entered[...] + arrived[...]
    partial[...] = jnp.dot(entering[...], even_turned[...], preferred_element_type=F32)


def forward_odd_kernel(partial, other, driving_even, driving_odd, odd_turned, _, even, odd):
    even[...] = (partial[...] + other[...] + driving_even[...]).astype(BF16)
    odd[...] = (jnp.dot(even[...], odd_turned[...], preferred_element_type=F32) + driving_odd[...]).astype(BF16)


def forward_first_kernel(driving_even, driving_odd, odd_turned, even, odd):
    even[...] = driving_even[...].astype(BF16)
    odd[...] = (jnp.dot(even[...], odd_turned[...], preferred_element_type=F32) + driving_odd[...]).astype(BF16)


def forward_last_kernel(entered, arrived, even_turned, partial):
    partial[...] = jnp.dot(entered[...] + arrived[...], even_turned[...], preferred_element_type=F32)


def backward_odd_last_kernel(entered, arrived, weight_odd, odd, odd_whole, _, adjoint_odd, partial):
    carry = (entered[...] + arrived[...]).astype(F32)
    adjoint_odd[...] = (weight_odd[...] * odd[...].astype(F32) + carry).astype(BF16)
    partial[...] = jnp.dot(adjoint_odd[...], odd_whole[...], preferred_element_type=F32)


def backward_even_last_kernel(partial, other, weight_even, even, _, adjoint_even):
    carry = partial[...] + other[...]
    adjoint_even[...] = (weight_even[...] * even[...].astype(F32) + carry).astype(BF16)


def backward_odd_kernel(entered, arrived, weight_odd, odd, odd_whole, _, entering, adjoint_odd, partial):
    entering[...] = entered[...] + arrived[...]
    adjoint_odd[...] = (weight_odd[...] * odd[...].astype(F32) + entering[...].astype(F32)).astype(BF16)
    partial[...] = jnp.dot(adjoint_odd[...], odd_whole[...], preferred_element_type=F32)


def backward_even_kernel(partial, other, weight_even, even, even_whole, _, adjoint_even, leaving):
    carry = partial[...] + other[...]
    adjoint_even[...] = (weight_even[...] * even[...].astype(F32) + carry).astype(BF16)
    leaving[...] = jnp.dot(adjoint_even[...], even_whole[...], preferred_element_type=F32).astype(BF16)


def pack_kernel(even, adjoint_even, odd, adjoint_odd, message):
    low = own_half() == 0
    blocks = even.shape[1] // 128

    def block(ref, i):
        return ref[:, 128 * i:128 * i + 128].astype(F32)

    for s in range(blocks):
        state, adjoint = block(even, s), block(adjoint_even, s)
        message[s] = jnp.where(low, joined(state, adjoint, True), joined(state, adjoint, False)).astype(BF16)
        message[blocks + s] = joined(block(odd, s // 2), block(adjoint_odd, s // 2), s % 2 == 0).astype(BF16)


def unpack_kernel(message, state, adjoint):
    for core in range(2):
        turned = message[core].astype(F32).T.astype(BF16)
        rows = pl.ds(pl.multiple_of((core + lax.axis_index("z")) % 2 * 64, 64), 64)
        state[0, rows, :] = turned[:64]
        adjoint[0, rows, :] = turned[64:]


def per_device(increments, propagators, inv_var):
    core = lax.axis_index("core")
    rows, wide = propagators.shape[1:]
    cols = increments.shape[2]
    members = Y * X
    own = cols // members
    half = wide // 2

    keep, give = call(split_kernel, [shape((rows, half))] * 2, [propagators[0]], "split")
    increments, inv_var, give = lax.optimization_barrier((increments, inv_var, give))
    taken = other_core(give)

    rest, parts = inv_var[0], []
    for _ in range(3):
        part = lax.reduce_precision(rest, 8, 7)
        parts.append(part.astype(BF16))
        rest = rest - part
    parts = jnp.broadcast_to(jnp.stack(parts)[None], (members, 3, rows))
    message = jnp.concatenate([increments[0].T.reshape(members, own, rows), parts], 1)
    messages = jnp.stack([message, other_core(message)], 1).reshape(Y, X, 2, own + 3, rows)
    messages, taken = lax.optimization_barrier((messages, taken))
    near, far = [], []
    for part, (first, second) in ((jnp.where(core == 0, keep, taken), ("y", "x")), (jnp.where(core == 0, taken, keep), ("x", "y"))):
        behind, ahead = ring(part, first, 1), ring(part, first, -1)
        if first == "y":
            came, behind, ahead = lax.optimization_barrier((exchanged(messages, "y"), behind, ahead))
            messages = jnp.stack(came, 0)
        columns = [slice(0, half // 2), slice(half // 2, half)]
        beyond = [ring(behind[:, columns[0]], first, 1), ring(ahead[:, columns[1]], first, -1)]
        for side in range(2):
            line = jnp.concatenate([block[:, columns[side]] for block in (part, behind, ahead)] + [beyond[side]], 0)
            if first == "x" and side == 1:
                messages, line = lax.optimization_barrier((messages, line))
                came = exchanged(messages, "x")
            after = [ring(line, second, 1), ring(line, second, -1)]
            near.append([line, *after])
            far.append(ring(after[side], second, 1 - 2 * side))
    near, far = near[2:] + near[:2], far[2:] + far[:2]
    before = assemble([piece for group in near for piece in group], (0, 1, 2), wide)
    came, before = lax.optimization_barrier((came, before))
    messages = jnp.stack(came, 1)
    wide_f32, half_f32 = shape((own, wide), F32), shape((own, half), F32)
    driving_even, driving_odd, weight_even, weight_odd = call(
        prepare_kernel, [wide_f32, half_f32, wide_f32, half_f32], [messages], "prepare",
        scratch=[pltpu.VMEM((own, wide), F32)] * 2)
    even_whole, odd_whole, even_turned, odd_turned = assemble(far, (3,), wide, before)

    full, part = shape((own, wide)), shape((own, half))
    costs = {"flops": int(2e9), "size": 4 * MIB}
    nothing = jnp.zeros((own, half), BF16)
    even, odd = call(forward_first_kernel, [full, part], [driving_even, driving_odd, odd_turned], "forward_first", **costs)
    entering, arrived = nothing, z_hop(odd, 0, 1)
    for step in range(1, Z):
        if step < Z - 1:
            entering, partial = call(forward_even_kernel, [part, wide_f32], [entering, arrived, even_turned], "forward_even", **costs)
        else:
            partial = call(forward_last_kernel, wide_f32, [entering, arrived, even_turned], "forward_last", **costs)
        even, odd = call(
            forward_odd_kernel, [full, part], [partial, other_core(partial), driving_even, driving_odd, odd_turned, even],
            "forward_odd", aliases={5: 0}, **costs)
        if step < Z - 1:
            arrived = z_hop(odd, step, step + 1)
    entering = arrived = nothing
    adjoint_even, adjoint_odd = jnp.zeros((own, wide), BF16), nothing
    for step in reversed(range(1, Z)):
        entering, adjoint_odd, partial = call(
            backward_odd_kernel, [part, part, wide_f32], [entering, arrived, weight_odd, odd, odd_whole, adjoint_odd],
            "backward_odd", aliases={5: 1}, **costs)
        adjoint_even, leaving = call(
            backward_even_kernel, [full, part], [partial, other_core(partial), weight_even, even, even_whole, adjoint_even],
            "backward_even", aliases={5: 0}, **costs)
        arrived = z_hop(leaving, step, step - 1)
    adjoint_odd, partial = call(
        backward_odd_last_kernel, [part, wide_f32], [entering, arrived, weight_odd, odd, odd_whole, adjoint_odd],
        "backward_odd_last", aliases={5: 0}, **costs)
    adjoint_even = call(
        backward_even_last_kernel, full, [partial, other_core(partial), weight_even, even, adjoint_even],
        "backward_even_last", aliases={4: 0})

    message = call(pack_kernel, shape((CORE * members, own, rows)), [even, adjoint_even, odd, adjoint_odd], "pack")
    message = lax.all_to_all(message, PLANE, split_axis=0, concat_axis=0, tiled=True)
    block = shape((1, rows, cols))
    return tuple(call(unpack_kernel, [block, block], [message.reshape(CORE, cols, rows)], "unpack"))


def solution(mesh):
    fine = Mesh(mesh.devices.reshape(Z, CORE, Y, X), ALL)
    tm, state = ("z", "core"), ("y", "x")
    in_specs = (P(tm, state, None), P(tm, state, None), P(tm, state))
    out_specs = (P(tm, state, None), P(tm, state, None))
    return jax.shard_map(per_device, mesh=fine, in_specs=in_specs, out_specs=out_specs, check_vma=False)
```

```python
import functools

import jax
import jax.numpy as jnp
from jax import lax
from jax.experimental import pallas as pl
from jax.experimental.pallas import tpu as pltpu
from jax.sharding import Mesh, PartitionSpec as P


Z, CORE, Y, X = 8, 2, 4, 4
PLANE = ("core", "y", "x")
ALL = ("z", "core", "y", "x")
MIB = 1 << 20
F32, BF16 = jnp.float32, jnp.bfloat16
OFFSETS = (0, -1, 1, 2)
VMEM = pl.BlockSpec(memory_space=pltpu.VMEM)
HBM = pl.BlockSpec(memory_space=pltpu.HBM)


def ring(block, axis, distance):
    n = lax.axis_size(axis)
    return lax.ppermute(block, axis, [(i, (i + distance) % n) for i in range(n)])


def z_hop(block, origin, target):
    size = Y * X
    return lax.ppermute(block, ALL, [
        ((origin * CORE + core) * size + i, (target * CORE + 1 - core) * size + i) for core in range(CORE) for i in range(size)])


def own_half():
    return (lax.axis_index("core") + lax.axis_index("z")) % 2


def other_core(block):
    return lax.ppermute(block, "core", [(0, 1), (1, 0)])


def exchanged(messages, axis):
    dim = ("y", "x").index(axis)
    came = []
    for distance in range(4):
        message = lax.dynamic_index_in_dim(messages, (lax.axis_index(axis) + distance) % 4, dim, keepdims=False)
        came.append(ring(message, axis, distance) if distance else message)
    return came


def call(kernel, results, operands, name, in_specs=None, flops=0, size=MIB, scratch=(), aliases=None):
    return pl.pallas_call(
        kernel,
        out_shape=results,
        in_specs=in_specs or [VMEM] * len(operands),
        out_specs=jax.tree.map(lambda _: VMEM, results),
        scratch_shapes=scratch,
        input_output_aliases=aliases or {},
        compiler_params=pltpu.CompilerParams(vmem_limit_bytes=4 * MIB),
        cost_estimate=pl.CostEstimate(flops=flops, bytes_accessed=size, transcendentals=0),
        name=name,
    )(*operands)


def shape(dims, dtype=BF16):
    return jax.ShapeDtypeStruct(dims, dtype)


def joined(left, right, low_half):
    lane = lax.broadcasted_iota(jnp.int32, left.shape, 1)
    if low_half:
        return jnp.where(lane < 64, left, pltpu.roll(right, 64, 1))
    return jnp.where(lane < 64, pltpu.roll(left, 64, 1), right)


def split_kernel(block, keep, give):
    rows, wide = block.shape
    half = wide // 2
    core, mine = lax.axis_index("core"), own_half()

    @pl.when(core == 1)
    def _():
        for target, which in ((keep, mine), (give, 1 - mine)):
            start = pl.ds(pl.multiple_of(which * 64, 64), 64)
            for side in range(2):
                target[side * 64:side * 64 + 64, :] = block[start, side * half:side * half + half]

    @pl.when(core == 0)
    def _():
        for u in range(wide // 256):
            left = block[:, 256 * u:256 * u + 128].astype(F32)
            right = block[:, 256 * u + 128:256 * u + 256].astype(F32)
            low, high = joined(left, right, True), joined(left, right, False)
            keep[:, 128 * u:128 * u + 128] = jnp.where(mine == 0, low, high).astype(BF16)
            give[:, 128 * u:128 * u + 128] = jnp.where(mine == 0, high, low).astype(BF16)


def assemble_kernel(fars, *refs):
    even, odd, even_turned, odd_turned, sems = refs[-5:]
    here = {axis: lax.axis_index(axis) for axis in PLANE}
    copies = []

    def copy(source, target):
        copies.append(pltpu.make_async_copy(source, target, sems.at[len(copies)]))

    for quarter in range(4):
        first, second = ("x", "y") if quarter < 2 else ("y", "x")
        columns = (quarter % 2) * 512
        for j, far in enumerate(fars[quarter % 2]):
            piece = refs[quarter * 2 + j]
            for i in range(4):
                at = {first: (here[first] + OFFSETS[i] + 4) % 4, second: (here[second] + OFFSETS[far] + 4) % 4}
                s = at["y"] * X + at["x"]
                if quarter < 2:
                    for side in range(2):
                        copy(piece.at[pl.ds(i * 128 + side * 64, 64), :],
                             odd.at[pl.ds(pl.multiple_of(s * 64, 64), 64), pl.ds(side * 1024 + columns, 512)])
                else:
                    copy(piece.at[pl.ds(i * 128, 128), :],
                         even.at[pl.ds(pl.multiple_of(s * 128, 128), 128), pl.ds(columns, 512)])
    for c in copies:
        c.start()
    for c in copies:
        c.wait()

    def turn(whole, turned, block, column):
        rows = pl.ds(pl.multiple_of(block * 128, 128), 128)
        turned[column:column + 512, rows] = whole[rows, column:column + 512].T

    for side in range(2):
        for far in fars[side]:
            @pl.loop(0, 4)
            def _(n):
                turn(even, even_turned, n * X + (here["x"] + OFFSETS[far] + 4) % 4, side * 512)

            @pl.loop(0, 2)
            def _(n):
                for column in (side * 512, 1024 + side * 512):
                    turn(odd, odd_turned, (here["y"] + OFFSETS[far] + 4) % 4 * 2 + n, column)


def assemble(pieces, fars, wide, before=()):
    def kernel(*refs):
        assemble_kernel(fars, *refs[:len(pieces)], *refs[len(pieces) + len(before):])

    tall, flat = shape((wide, wide // 2)), shape((wide // 2, wide))
    return call(
        kernel, [tall, flat, flat, tall], [*pieces, *before], "assemble",
        in_specs=[HBM] * len(pieces) + [VMEM] * len(before), flops=int(2e9), size=len(pieces) * MIB,
        scratch=[pltpu.SemaphoreType.DMA((len(pieces) * 6,))], aliases={len(pieces) + i: i for i in range(len(before))})


def prepare_kernel(messages, driving_even, driving_odd, weight_even, weight_odd, driving, weight):
    even_first, low = lax.axis_index("core") == 0, own_half() == 0
    y, x = lax.axis_index("y"), lax.axis_index("x")
    for i in range(Y):
        for j in range(X):
            s = (y - i + Y) % Y * X + (x - j + X) % X
            lanes = pl.ds(pl.multiple_of(s * 128, 128), 128)
            own, other = messages[i, j, 0].astype(F32), messages[i, j, 1].astype(F32)
            for block, to_driving, to_weight in ((jnp.where(even_first, own, other), driving_even, weight_even),
                                                 (jnp.where(even_first, other, own), driving, weight)):
                to_driving[:, lanes] = block[:8]
                to_weight[:, lanes] = jnp.broadcast_to(block[8:9] + block[9:10] + block[10:11], (8, 128))
    for source, target in ((driving, driving_odd), (weight, weight_odd)):
        for u in range(target.shape[1] // 128):
            left, right = source[:, 256 * u:256 * u + 128], source[:, 256 * u + 128:256 * u + 256]
            target[:, 128 * u:128 * u + 128] = jnp.where(low, joined(left, right, True), joined(left, right, False))


def forward_even_kernel(entered, arrived, even_turned, entering, partial):
    entering[...] = entered[...] + arrived[...]
    partial[...] = jnp.dot(entering[...], even_turned[...], preferred_element_type=F32)


def forward_odd_kernel(partial, other, driving_even, driving_odd, odd_turned, _, even, odd):
    even[...] = (partial[...] + other[...] + driving_even[...]).astype(BF16)
    odd[...] = (jnp.dot(even[...], odd_turned[...], preferred_element_type=F32) + driving_odd[...]).astype(BF16)


def forward_first_kernel(driving_even, driving_odd, odd_turned, even, odd):
    even[...] = driving_even[...].astype(BF16)
    odd[...] = (jnp.dot(even[...], odd_turned[...], preferred_element_type=F32) + driving_odd[...]).astype(BF16)


def forward_last_kernel(entered, arrived, even_turned, partial):
    partial[...] = jnp.dot(entered[...] + arrived[...], even_turned[...], preferred_element_type=F32)


def backward_odd_last_kernel(entered, arrived, weight_odd, odd, odd_whole, _, adjoint_odd, partial):
    carry = (entered[...] + arrived[...]).astype(F32)
    adjoint_odd[...] = (weight_odd[...] * odd[...].astype(F32) + carry).astype(BF16)
    partial[...] = jnp.dot(adjoint_odd[...], odd_whole[...], preferred_element_type=F32)


def backward_even_last_kernel(partial, other, weight_even, even, _, adjoint_even):
    carry = partial[...] + other[...]
    adjoint_even[...] = (weight_even[...] * even[...].astype(F32) + carry).astype(BF16)


def backward_odd_kernel(entered, arrived, weight_odd, odd, odd_whole, _, entering, adjoint_odd, partial):
    entering[...] = entered[...] + arrived[...]
    adjoint_odd[...] = (weight_odd[...] * odd[...].astype(F32) + entering[...].astype(F32)).astype(BF16)
    partial[...] = jnp.dot(adjoint_odd[...], odd_whole[...], preferred_element_type=F32)


def backward_even_kernel(partial, other, weight_even, even, even_whole, _, adjoint_even, leaving):
    carry = partial[...] + other[...]
    adjoint_even[...] = (weight_even[...] * even[...].astype(F32) + carry).astype(BF16)
    leaving[...] = jnp.dot(adjoint_even[...], even_whole[...], preferred_element_type=F32).astype(BF16)


def pack_kernel(even, adjoint_even, odd, adjoint_odd, message):
    low = own_half() == 0
    blocks = even.shape[1] // 128

    def block(ref, i):
        return ref[:, 128 * i:128 * i + 128].astype(F32)

    for s in range(blocks):
        state, adjoint = block(even, s), block(adjoint_even, s)
        message[s] = jnp.where(low, joined(state, adjoint, True), joined(state, adjoint, False)).astype(BF16)
        message[blocks + s] = joined(block(odd, s // 2), block(adjoint_odd, s // 2), s % 2 == 0).astype(BF16)


def unpack_kernel(message, state, adjoint):
    for core in range(2):
        turned = message[core].astype(F32).T.astype(BF16)
        rows = pl.ds(pl.multiple_of((core + lax.axis_index("z")) % 2 * 64, 64), 64)
        state[0, rows, :] = turned[:64]
        adjoint[0, rows, :] = turned[64:]


def per_device(increments, propagators, inv_var):
    core = lax.axis_index("core")
    rows, wide = propagators.shape[1:]
    cols = increments.shape[2]
    members = Y * X
    own = cols // members
    half = wide // 2

    keep, give = call(split_kernel, [shape((rows, half))] * 2, [propagators[0]], "split")
    increments, inv_var, give = lax.optimization_barrier((increments, inv_var, give))
    taken = other_core(give)

    rest, parts = inv_var[0], []
    for _ in range(3):
        part = lax.reduce_precision(rest, 8, 7)
        parts.append(part.astype(BF16))
        rest = rest - part
    parts = jnp.broadcast_to(jnp.stack(parts)[None], (members, 3, rows))
    message = jnp.concatenate([increments[0].T.reshape(members, own, rows), parts], 1)
    messages = jnp.stack([message, other_core(message)], 1).reshape(Y, X, 2, own + 3, rows)
    messages, taken = lax.optimization_barrier((messages, taken))
    near, far = [], []
    for part, (first, second) in ((jnp.where(core == 0, keep, taken), ("y", "x")), (jnp.where(core == 0, taken, keep), ("x", "y"))):
        behind, ahead = ring(part, first, 1), ring(part, first, -1)
        if first == "y":
            came, behind, ahead = lax.optimization_barrier((exchanged(messages, "y"), behind, ahead))
            messages = jnp.stack(came, 0)
        columns = [slice(0, half // 2), slice(half // 2, half)]
        beyond = [ring(behind[:, columns[0]], first, 1), ring(ahead[:, columns[1]], first, -1)]
        for side in range(2):
            line = jnp.concatenate([block[:, columns[side]] for block in (part, behind, ahead)] + [beyond[side]], 0)
            if first == "x" and side == 1:
                messages, line = lax.optimization_barrier((messages, line))
                came = exchanged(messages, "x")
            after = [ring(line, second, 1), ring(line, second, -1)]
            near.append([line, *after])
            far.append(ring(after[side], second, 1 - 2 * side))
    near, far = near[2:] + near[:2], far[2:] + far[:2]
    early, late = ((0, 1), (0, 2)), ((2, 3), (1, 3))
    every = [[*near[i], far[i]] for i in range(4)]
    before = assemble([every[i][n] for i in range(4) for n in early[i % 2]], early, wide)
    came, before = lax.optimization_barrier((came, before))
    messages = jnp.stack(came, 1)
    wide_f32, half_f32 = shape((own, wide), F32), shape((own, half), F32)
    driving_even, driving_odd, weight_even, weight_odd = call(
        prepare_kernel, [wide_f32, half_f32, wide_f32, half_f32], [messages], "prepare",
        scratch=[pltpu.VMEM((own, wide), F32)] * 2)
    even_whole, odd_whole, even_turned, odd_turned = assemble([every[i][n] for i in range(4) for n in late[i % 2]], late, wide, before)

    full, part = shape((own, wide)), shape((own, half))
    costs = {"flops": int(2e9), "size": 4 * MIB}
    nothing = jnp.zeros((own, half), BF16)
    even, odd = call(forward_first_kernel, [full, part], [driving_even, driving_odd, odd_turned], "forward_first", **costs)
    entering, arrived = nothing, z_hop(odd, 0, 1)
    for step in range(1, Z):
        if step < Z - 1:
            entering, partial = call(forward_even_kernel, [part, wide_f32], [entering, arrived, even_turned], "forward_even", **costs)
        else:
            partial = call(forward_last_kernel, wide_f32, [entering, arrived, even_turned], "forward_last", **costs)
        even, odd = call(
            forward_odd_kernel, [full, part], [partial, other_core(partial), driving_even, driving_odd, odd_turned, even],
            "forward_odd", aliases={5: 0}, **costs)
        if step < Z - 1:
            arrived = z_hop(odd, step, step + 1)
    entering = arrived = nothing
    adjoint_even, adjoint_odd = jnp.zeros((own, wide), BF16), nothing
    for step in reversed(range(1, Z)):
        entering, adjoint_odd, partial = call(
            backward_odd_kernel, [part, part, wide_f32], [entering, arrived, weight_odd, odd, odd_whole, adjoint_odd],
            "backward_odd", aliases={5: 1}, **costs)
        adjoint_even, leaving = call(
            backward_even_kernel, [full, part], [partial, other_core(partial), weight_even, even, even_whole, adjoint_even],
            "backward_even", aliases={5: 0}, **costs)
        arrived = z_hop(leaving, step, step - 1)
    adjoint_odd, partial = call(
        backward_odd_last_kernel, [part, wide_f32], [entering, arrived, weight_odd, odd, odd_whole, adjoint_odd],
        "backward_odd_last", aliases={5: 0}, **costs)
    adjoint_even = call(
        backward_even_last_kernel, full, [partial, other_core(partial), weight_even, even, adjoint_even],
        "backward_even_last", aliases={4: 0})

    message = call(pack_kernel, shape((CORE * members, own, rows)), [even, adjoint_even, odd, adjoint_odd], "pack")
    message = lax.all_to_all(message, PLANE, split_axis=0, concat_axis=0, tiled=True)
    block = shape((1, rows, cols))
    return tuple(call(unpack_kernel, [block, block], [message.reshape(CORE, cols, rows)], "unpack"))


def solution(mesh):
    fine = Mesh(mesh.devices.reshape(Z, CORE, Y, X), ALL)
    tm, state = ("z", "core"), ("y", "x")
    in_specs = (P(tm, state, None), P(tm, state, None), P(tm, state))
    out_specs = (P(tm, state, None), P(tm, state, None))
    return jax.shard_map(per_device, mesh=fine, in_specs=in_specs, out_specs=out_specs, check_vma=False)
```
